128 devices in a mesh: data: 1, model: 128 (over z, y, x, core).
Axes of the slice: x: 4, y: 4, z: 4, core: 2. Of those that a mesh axis runs over, the one named last changes fastest.
Arguments:
- queries: bfloat16 [32, 2048], P('data')
- w_head: bfloat16 [2048, 32000], P(None, 'model')
- ds_keys: bfloat16 [262144, 2048], P('model')
- ds_tokens: int32 [262144], P('model')
- temperature: float32 [1], replicated
- mix_weight: float32 [1], replicated
Outputs:
- output: float32 [32, 32000], P('data', 'model')
All inputs are finite; a program needn't handle non-finite values.
Results may differ from the reference program's by a relative error of at most 0.001.
Values are sent between devices in bfloat16 or wider.
A program may use at most 1 GiB of HBM per device.

```python
import jax
import jax.numpy as jnp
from jax import lax

Q_ROWS = 32
D_MODEL = 2048
VOCAB_SIZE = 32000
N_LOCAL = 2048
GROUP_SIZE = 128


def setup_inputs(seed: int = 0, part: int = 0) -> dict:
    root_key = jax.random.key(seed)
    key_query, key_head, key_store, key_token, key_temp, key_mix = jax.random.split(root_key, 6)
    key_query = jax.random.fold_in(key_query, part)
    n_total = GROUP_SIZE * N_LOCAL
    queries = jax.random.normal(key_query, (Q_ROWS, D_MODEL), jnp.float32)
    w_head = jax.random.normal(key_head, (D_MODEL, VOCAB_SIZE), jnp.float32) * (2.0 * D_MODEL ** -0.5)
    ds_keys = jax.random.normal(key_store, (n_total, D_MODEL), jnp.float32)
    ds_tokens = jax.random.randint(key_token, (n_total,), 0, VOCAB_SIZE, jnp.int32)
    ds_tokens = ds_tokens.at[0].set(VOCAB_SIZE - 1).at[1].set(0)
    temperature = jax.random.uniform(key_temp, (1,), jnp.float32, 0.7, 0.95) * (D_MODEL ** 0.5)
    mix_weight = jax.random.uniform(key_mix, (1,), jnp.float32, 0.25, 0.5)
    return {
        "queries": queries.astype(jnp.bfloat16),
        "w_head": w_head.astype(jnp.bfloat16),
        "ds_keys": ds_keys.astype(jnp.bfloat16),
        "ds_tokens": ds_tokens,
        "temperature": temperature,
        "mix_weight": mix_weight,
    }


def reference(queries, w_head, ds_keys, ds_tokens, temperature, mix_weight):
    key_blocks = ds_keys.reshape(GROUP_SIZE, N_LOCAL, D_MODEL)
    tok_blocks = ds_tokens.reshape(GROUP_SIZE, N_LOCAL)
    temp_value = temperature[0]

    def block_scores(key_block):
        cross_dot = jnp.dot(queries, key_block.T, preferred_element_type=jnp.float32)
        key_sq = jnp.sum(jnp.square(key_block.astype(jnp.float32)), axis=1)
        return (2.0 * cross_dot - key_sq[None, :]) / temp_value

    block_max = lax.map(lambda key_block: jnp.max(block_scores(key_block), axis=1), key_blocks)
    row_max = jnp.max(block_max, axis=0)

    def accumulate(carry_state, block_pair):
        histogram, row_total = carry_state
        key_block, tok_block = block_pair
        weights = jnp.exp(block_scores(key_block) - row_max[:, None])
        histogram = histogram.at[:, tok_block].add(weights)
        return (histogram, row_total + jnp.sum(weights, axis=1)), None

    start_state = (jnp.zeros((Q_ROWS, VOCAB_SIZE), jnp.float32), jnp.zeros((Q_ROWS,), jnp.float32))
    (histogram, row_total), unused = lax.scan(accumulate, start_state, (key_blocks, tok_blocks))
    logits = jnp.dot(queries, w_head, preferred_element_type=jnp.float32)
    lm_exp = jnp.exp(logits - jnp.max(logits, axis=1, keepdims=True))
    p_lm = lm_exp / jnp.sum(lm_exp, axis=1, keepdims=True)
    mix_value = mix_weight[0]
    return jnp.log(mix_value * histogram / row_total[:, None] + (1.0 - mix_value) * p_lm)
```

```python
import functools

import jax
import jax.numpy as jnp
from jax import lax
from jax.experimental import pallas as pl
from jax.experimental.pallas import tpu as pltpu
from jax.sharding import PartitionSpec as P

MESH = pl.DeviceIdType.MESH
F32 = jnp.float32
BF16 = jnp.bfloat16
LANES = 128
ROWS = 11
CAP = 4 * ROWS
STAT = 64
COUNT = 48
EMPTY = 255.0


def _iota(shape, dim):
    return lax.broadcasted_iota(jnp.int32, shape, dim).astype(F32)


def _split3(x):
    hi = x.astype(BF16)
    rest = x - hi.astype(F32)
    mid = rest.astype(BF16)
    low = (rest - mid.astype(F32)).astype(BF16)
    return hi, mid, low


def _kernel(
    n_dev, rnd_ref, tau_ref, mix_ref, q_hbm, w_hbm, key_hbm, tok_hbm,
    p_ref, plm_ref, cnt_ref,
    q_ref, w_ref, key_ref, tok_ref, hot_ref, pack_ref, rhs_ref, s_ref, mask_ref, send, recv, x_ref,
    in_sem, key_sem, send_sem, recv_sem,
):
    me = lax.axis_index("model")
    n_rows, dim = q_ref.shape
    n_keys = key_ref.shape[0]
    v_loc = w_ref.shape[1]
    n_blk = n_keys // LANES
    n_chunk = key_sem.shape[0]
    step = n_keys // n_chunk

    loads = [
        pltpu.make_async_copy(src, dst, in_sem.at[i])
        for i, (src, dst) in enumerate([(tok_hbm, tok_ref), (q_hbm, q_ref), (w_hbm, w_ref)])
    ]
    loads += [
        pltpu.make_async_copy(key_hbm.at[pl.ds(i * step, step)], key_ref.at[pl.ds(i * step, step)], key_sem.at[i])
        for i in range(n_chunk)
    ]
    for load in loads:
        load.start()

    barrier = pltpu.get_barrier_semaphore()

    def greet(o, carry):
        pl.semaphore_signal(barrier, inc=1, device_id={"model": lax.rem(me + o, n_dev)}, device_id_type=MESH)
        return carry

    lax.fori_loop(1, n_dev, greet, 0)

    loads[0].wait()
    tok = tok_ref[...].astype(F32)
    owner = jnp.floor((tok + 0.5) * (1.0 / v_loc))
    place = tok - owner * v_loc + 1.0
    sub = _iota((LANES, LANES), 0)
    lane = _iota((LANES, LANES), 1)
    for c in range(n_blk):
        hot_ref[:, c * LANES : (c + 1) * LANES] = jnp.where(sub == owner[c : c + 1, :], 1.0, 0.0).astype(BF16)
    ones = jnp.ones((LANES, LANES), BF16)
    upper = jnp.where(sub <= lane, 1.0, 0.0).astype(BF16)
    tri = jnp.concatenate([upper, ones], axis=1)
    hot_rows = jnp.concatenate([hot_ref[:, c * LANES : (c + 1) * LANES] for c in range(n_blk)], axis=0)
    ranks = jnp.dot(hot_rows, tri, preferred_element_type=F32)
    before = jnp.zeros((LANES, LANES), F32)
    first = rnd_ref[0].astype(F32) * float(CAP) + 1.0
    for c in range(n_blk):
        part = ranks[c * LANES : (c + 1) * LANES]
        mine = sub == owner[c : c + 1, :]
        slot = jnp.sum(jnp.where(mine, part[:, :LANES] + before, 0.0), axis=0, keepdims=True) - first
        before = before + part[:, LANES:]
        slot = jnp.where((slot >= 0.0) & (slot < float(CAP)), slot, EMPTY)
        diag = sub == lane
        slot_col = jnp.dot(jnp.where(diag, slot, 0.0).astype(BF16), ones, preferred_element_type=F32)
        place_col = jnp.dot(
            jnp.where(diag, place[c : c + 1, :], 0.0).astype(BF16), ones, preferred_element_type=F32
        )
        rows = pl.ds(c * LANES, LANES)
        rhs_ref[rows, 0:LANES] = jnp.where(slot_col == lane, place_col, 0.0).astype(BF16)
        mask_ref[rows, :] = slot_col - 4.0 * jnp.floor(slot_col * 0.25)
        code = owner[c : c + 1, :] + LANES * jnp.floor(slot * 0.25)
        for r in range(ROWS):
            pack_ref[r * LANES : (r + 1) * LANES, c * LANES : (c + 1) * LANES] = jnp.where(
                sub + float(r * LANES) == code, 1.0, 0.0
            ).astype(BF16)
    meta = jnp.dot(hot_ref[...], rhs_ref[:, 0:LANES], preferred_element_type=F32)
    biggest = jnp.max(before, axis=0, keepdims=True)

    loads[1].wait()
    loads[2].wait()
    q = q_ref[...]
    logits = jnp.dot(q, w_ref[...], preferred_element_type=F32)
    lm_max = jnp.max(logits, axis=1, keepdims=True)
    lm_lse = lm_max + jnp.log(jnp.sum(jnp.exp(logits - lm_max), axis=1, keepdims=True))
    q_sub = _iota((n_rows, LANES), 0)
    q_lane = _iota((n_rows, LANES), 1)
    lse_row = jnp.sum(jnp.where(q_lane == q_sub + float(STAT + 32), lm_lse, 0.0), axis=0, keepdims=True)

    q4 = jnp.concatenate([q, q, q, q], axis=0)
    inv_tau = 1.0 / jnp.full((1, LANES), tau_ref[0], F32)
    top = jnp.full((1, LANES), -jnp.inf, F32)
    for i in range(n_chunk):
        loads[3 + i].wait()
        rows = pl.ds(i * step, step)
        dots = lax.dot_general(key_ref[rows, :], q4, (((1,), (1,)), ((), ())), preferred_element_type=F32)
        sq = jnp.zeros((step, LANES), F32)
        for t in range(dim // LANES):
            k = key_ref[rows, t * LANES : (t + 1) * LANES].astype(F32)
            sq = sq + k * k
        s = (2.0 * dots - jnp.sum(sq, axis=1, keepdims=True)) * inv_tau
        s_ref[rows, :] = s
        top = jnp.maximum(top, jnp.max(s, axis=0, keepdims=True))
    total = jnp.zeros((1, LANES), F32)
    for i in range(n_chunk):
        rows = pl.ds(i * step, step)
        e = jnp.exp(s_ref[rows, :] - top)
        s_ref[rows, :] = e
        total = total + jnp.sum(e, axis=0, keepdims=True)
    scale = 1.0 / total
    knn_lse = top + jnp.log(total)
    group = jnp.floor(_iota((step, LANES), 1) * (1.0 / 32.0))
    for i in range(n_chunk):
        rows = pl.ds(i * step, step)
        parts = _split3(jnp.where(mask_ref[rows, :] == group, s_ref[rows, :] * scale, 0.0))
        for k in range(3):
            rhs_ref[rows, k * LANES : (k + 1) * LANES] = parts[k]

    packed = jnp.dot(pack_ref[...], rhs_ref[...], preferred_element_type=F32)
    packed = packed[:, :LANES] + packed[:, LANES : 2 * LANES] + packed[:, 2 * LANES :]
    for r in range(ROWS):
        send[r] = packed[r * LANES : (r + 1) * LANES]
    row_lane = _iota((1, LANES), 1)
    stats = jnp.where((row_lane >= float(STAT)) & (row_lane < float(STAT + 32)), knn_lse, lse_row)
    stats = jnp.where(row_lane == float(COUNT), biggest, stats)
    send[ROWS] = meta + stats

    pl.semaphore_wait(barrier, n_dev - 1)

    def push(o, carry):
        to = lax.rem(me + o * 37, n_dev)
        pltpu.make_async_remote_copy(
            send.at[:, to], recv.at[:, me], send_sem, recv_sem, device_id={"model": to}, device_id_type=MESH
        ).start()
        return carry

    lax.fori_loop(1, n_dev, push, 0)
    recv[:, pl.ds(me, 1), :] = send[:, pl.ds(me, 1), :]
    others = recv.at[:, pl.ds(0, n_dev - 1)]
    pltpu.make_async_copy(others, others, recv_sem).wait()

    meta = recv[ROWS]
    peak = jnp.max(meta, axis=0, keepdims=True)
    grown = jnp.exp(meta - peak)
    sums = jnp.sum(grown, axis=0, keepdims=True)
    in_knn = (lane >= float(STAT)) & (lane < float(STAT + 32))
    share = jnp.where(in_knn, grown * (mix_ref[0] / sums), 0.0)
    share = share + pltpu.roll(share, 64, 1)
    share = share + pltpu.roll(share, 32, 1)
    lse = peak + jnp.log(sums)
    lse_col = jnp.sum(jnp.where(q_lane == q_sub + float(STAT + 32), lse, 0.0), axis=1, keepdims=True)
    plm_ref[...] = (1.0 - mix_ref[0]) * jnp.exp(logits - lse_col)
    cnt_ref[...] = jnp.broadcast_to(jnp.max(jnp.where(row_lane == float(COUNT), peak, 0.0), axis=1, keepdims=True), (1, LANES))

    for r in range(ROWS):
        parts = _split3(recv[r] * share)
        for k in range(3):
            x_ref[r * LANES : (r + 1) * LANES, k * LANES : (k + 1) * LANES] = parts[k]
    places = jnp.transpose(meta)
    vocab = _iota((2 * LANES, LANES), 0) + 1.0
    vgroup = jnp.floor(_iota((2 * LANES, LANES), 1) * (1.0 / 32.0))
    acc = jnp.zeros((2 * LANES, LANES), F32)
    for j in range(4):
        hot = jnp.concatenate(
            [jnp.where(vocab == places[4 * r + j : 4 * r + j + 1, :], 1.0, 0.0).astype(BF16) for r in range(ROWS)], axis=1
        )
        h = jnp.dot(hot, x_ref[...], preferred_element_type=F32)
        h = h[:, :LANES] + h[:, LANES : 2 * LANES] + h[:, 2 * LANES :]
        acc = jnp.where(vgroup == float(j), h, acc)
    flat = jnp.transpose(acc)
    p = flat[0:32] + flat[32:64] + flat[64:96] + flat[96:128]
    p_ref[...] = p[:, :v_loc]

    mine = send.at[:, pl.ds(0, n_dev - 1)]
    pltpu.make_async_copy(mine, mine, send_sem).wait()


def solution(mesh):
    n_dev = mesh.shape["model"]

    def local_step(queries, w_shard, key_shard, tok_shard, temperature, mix_weight):
        n_rows, dim = queries.shape
        n_keys, v_loc = key_shard.shape[0], w_shard.shape[1]
        tok = tok_shard.reshape(n_keys // LANES, LANES)
        any_space = pl.BlockSpec(memory_space=pl.ANY)
        smem = pl.BlockSpec(memory_space=pltpu.SMEM)
        vmem = pl.BlockSpec(memory_space=pltpu.VMEM)
        n_chunk = 8
        exchange = pl.pallas_call(
            functools.partial(_kernel, n_dev),
            out_shape=[
                jax.ShapeDtypeStruct((n_rows, v_loc), F32),
                jax.ShapeDtypeStruct((n_rows, v_loc), F32),
                jax.ShapeDtypeStruct((1, LANES), F32),
            ],
            in_specs=[smem, smem, smem, any_space, any_space, any_space, any_space],
            out_specs=[vmem, vmem, vmem],
            scratch_shapes=[
                pltpu.VMEM((n_rows, dim), BF16),
                pltpu.VMEM((dim, v_loc), BF16),
                pltpu.VMEM((n_keys, dim), BF16),
                pltpu.VMEM((n_keys // LANES, LANES), jnp.int32),
                pltpu.VMEM((n_dev, n_keys), BF16),
                pltpu.VMEM((ROWS * n_dev, n_keys), BF16),
                pltpu.VMEM((n_keys, 3 * LANES), BF16),
                pltpu.VMEM((n_keys, LANES), F32),
                pltpu.VMEM((n_keys, LANES), F32),
                pltpu.VMEM((ROWS + 1, n_dev, LANES), F32),
                pltpu.VMEM((ROWS + 1, n_dev, LANES), F32),
                pltpu.VMEM((ROWS * n_dev, 3 * LANES), BF16),
                pltpu.SemaphoreType.DMA((3,)),
                pltpu.SemaphoreType.DMA((n_chunk,)),
                pltpu.SemaphoreType.DMA,
                pltpu.SemaphoreType.DMA,
            ],
            compiler_params=pltpu.CompilerParams(
                collective_id=0, has_side_effects=True, vmem_limit_bytes=60 * 1024 * 1024
            ),
        )

        def run(r):
            return exchange(r.reshape(1), temperature, mix_weight, queries, w_shard, key_shard, tok)

        p_knn, p_lm, count = run(jnp.int32(0))
        rounds = lax.div(count[0, 0].astype(jnp.int32) + (CAP - 1), CAP)

        def more(state):
            return state[0] + 1, state[1] + run(state[0])[0]

        p_knn = lax.while_loop(lambda state: state[0] < rounds, more, (jnp.int32(1), p_knn))[1]
        return jnp.log(p_knn + p_lm)

    return jax.shard_map(
        local_step,
        mesh=mesh,
        in_specs=(P("data", None), P(None, "model"), P("model", None), P("model"), P(), P()),
        out_specs=P("data", "model"),
        check_vma=False,
    )
```

```python
import functools

import jax
import jax.numpy as jnp
from jax import lax
from jax.experimental import pallas as pl
from jax.experimental.pallas import tpu as pltpu
from jax.sharding import PartitionSpec as P

MESH = pl.DeviceIdType.MESH
F32 = jnp.float32
BF16 = jnp.bfloat16
LANES = 128
WIDE = 2 * LANES
DEPTH = 4
CAP = 8 * DEPTH
POOL = 4
ROWS = 2 * DEPTH + 1
PARTS = 2
HALF = 2
COUNT = 48
STAT = 64
EMPTY = 255.0


def _iota(shape, dim):
    return lax.broadcasted_iota(jnp.int32, shape, dim).astype(F32)


def _split3(x):
    hi = x.astype(BF16)
    rest = x - hi.astype(F32)
    mid = rest.astype(BF16)
    low = (rest - mid.astype(F32)).astype(BF16)
    return hi, mid, low


def _bucket(owner, source, n_dev):
    ahead = owner - source
    ahead = jnp.where(ahead < 0.0, ahead + float(n_dev), ahead)
    turn = jnp.floor(ahead * (1.0 / PARTS))
    return (ahead - PARTS * turn) * float(n_dev // PARTS) + turn


def _kernel(n_dev, whole, rnd_ref, tau_hbm, mix_hbm, q_hbm, w_hbm, key_hbm, tok_hbm, *refs):
    outs, refs = (refs[:2], refs[2:]) if whole else (refs[:3], refs[3:])
    (
        tau_ref, mix_ref, q_ref, w_ref, key_ref, tok_ref, hot_ref, pack_ref, place_ref, rhs_ref, s_ref, mask_ref,
        send, recv, x_ref, found_ref, in_sem, key_sem, send_sem, recv_sem,
    ) = refs
    me = lax.axis_index("model")
    me_f = me.astype(F32)
    n_rows, dim = q_ref.shape
    n_keys = key_ref.shape[0]
    v_loc = w_ref.shape[1]
    n_blk = n_keys // LANES
    n_chunk = key_sem.shape[0]
    step = n_keys // n_chunk
    group_len = n_dev // PARTS
    half_len = n_dev // HALF
    pool_at = DEPTH * group_len

    sources = [(tok_hbm, tok_ref), (q_hbm, q_ref), (w_hbm, w_ref), (tau_hbm, tau_ref), (mix_hbm, mix_ref)]
    loads = [pltpu.make_async_copy(src, dst, in_sem.at[i]) for i, (src, dst) in enumerate(sources)]
    key_loads = [
        pltpu.make_async_copy(key_hbm.at[pl.ds(i * step, step)], key_ref.at[pl.ds(i * step, step)], key_sem.at[i])
        for i in range(n_chunk)
    ]
    for load in loads + key_loads:
        load.start()

    barrier = pltpu.get_barrier_semaphore()
    for o in range(1, n_dev):
        pl.semaphore_signal(barrier, inc=1, device_id={"model": lax.rem(me + o, n_dev)}, device_id_type=MESH)

    loads[0].wait()
    tok = tok_ref[...].astype(F32)
    owner = jnp.floor((tok + 0.5) * (1.0 / v_loc))
    place = tok - owner * v_loc + 1.0
    bucket = _bucket(owner, me_f, n_dev)
    sub = _iota((LANES, LANES), 0)
    lane = _iota((LANES, LANES), 1)
    diag = sub == lane
    ones = jnp.ones((LANES, LANES), BF16)
    upper = jnp.where(sub <= lane, 1.0, 0.0).astype(BF16)
    tri = jnp.concatenate([upper, ones], axis=1)
    for c in range(n_blk):
        hot_ref[:, c * LANES : (c + 1) * LANES] = jnp.where(sub == bucket[c : c + 1, :], 1.0, 0.0).astype(BF16)
    ranks = []
    for c in range(0, n_blk, 4):
        hot_rows = jnp.concatenate([hot_ref[:, k * LANES : (k + 1) * LANES] for k in range(c, c + 4)], axis=0)
        part = jnp.dot(hot_rows, tri, preferred_element_type=F32)
        ranks += [part[k * LANES : (k + 1) * LANES] for k in range(4)]
    before = jnp.zeros((LANES, LANES), F32)
    first = 1.0 if whole else rnd_ref[0].astype(F32) * float(CAP) + 1.0
    slots = []
    for c in range(n_blk):
        mine = sub == bucket[c : c + 1, :]
        slots.append(jnp.sum(jnp.where(mine, ranks[c][:, :LANES] + before, 0.0), axis=0, keepdims=True) - first)
        before = before + ranks[c][:, LANES:]
    slot = jnp.concatenate(slots, axis=0)
    if whole:
        over = jnp.where(slot >= float(CAP), 1.0, 0.0)
        inside = jnp.dot(over.astype(BF16), tri, preferred_element_type=F32)
        lower = jnp.where(_iota((n_blk, n_blk), 0) > _iota((n_blk, n_blk), 1), 1.0, 0.0).astype(BF16)
        ahead = jnp.dot(lower, inside[:, LANES:].astype(BF16), preferred_element_type=F32)
        rank = ahead + inside[:, :LANES] - 1.0
        code = jnp.where(rank < float(POOL), rank + float(CAP), EMPTY)
        code = jnp.where(slot < float(CAP), slot, code)
        demand = (ahead + inside[:, LANES:])[n_blk - 1 : n_blk]
    else:
        code = jnp.where((slot >= 0.0) & (slot < float(CAP)), slot, EMPTY)
        demand = jnp.max(before, axis=0, keepdims=True)
    depth = jnp.floor(code * 0.125)
    lane_group = jnp.floor(lane * (1.0 / 32.0))

    def sort_block(c):
        rows = pl.ds(c * LANES, LANES)
        cols = slice(c * LANES, (c + 1) * LANES)
        both = jnp.concatenate(
            [jnp.where(diag, code[c : c + 1, :], 0.0), jnp.where(diag, place[c : c + 1, :], 0.0)], axis=0
        )
        both = jnp.dot(both.astype(BF16), ones, preferred_element_type=F32)
        code_col, place_col = both[:LANES], both[LANES:]
        place_ref[rows, :] = jnp.where(code_col == lane, place_col, 0.0).astype(BF16)
        eighth = code_col - 8.0 * jnp.floor(code_col * 0.125)
        mask_ref[rows, :LANES] = jnp.where(eighth == lane_group, 1.0, 0.0).astype(BF16)
        mask_ref[rows, LANES:] = jnp.where(eighth == lane_group + 4.0, 1.0, 0.0).astype(BF16)
        hot = hot_ref[:, cols]
        for r in range(DEPTH):
            keep = jnp.broadcast_to(jnp.where(depth[c : c + 1, :] == float(r), 1.0, 0.0), (LANES, LANES)).astype(BF16)
            kept = hot * keep
            for g in range(PARTS):
                at = g * (pool_at + 16) + r * group_len
                pack_ref[at : at + group_len, cols] = kept[g * group_len : (g + 1) * group_len]
        spare = jnp.where((depth[c : c + 1, :] == float(DEPTH)) & (_iota((16, LANES), 0) == 0.0), 1.0, 0.0)
        pack_ref[pool_at : pool_at + 16, cols] = spare.astype(BF16)

    for load in loads[1:]:
        load.wait()
    q = q_ref[...]
    logits = jnp.dot(q, w_ref[...], preferred_element_type=F32)
    lm_max = jnp.max(logits, axis=1, keepdims=True)
    lm_lse = lm_max + jnp.log(jnp.sum(jnp.exp(logits - lm_max), axis=1, keepdims=True))
    q_sub = _iota((n_rows, LANES), 0)
    q_lane = _iota((n_rows, LANES), 1)
    knn_diag = q_lane == q_sub + float(STAT)
    lm_diag = q_lane == q_sub + float(STAT + 32)
    lse_row = jnp.sum(jnp.where(lm_diag, lm_lse, 0.0), axis=0, keepdims=True)

    q4 = jnp.concatenate([q, q, q, q], axis=0)
    inv_tau = 1.0 / jnp.full((1, LANES), tau_ref[0], F32)
    tops, totals = [], []
    fine = step // 2
    for i in range(n_chunk):
        key_loads[i].wait()
        for c in range(i * n_blk // n_chunk, (i + 1) * n_blk // n_chunk):
            sort_block(c)
        for j in range(2):
            rows = pl.ds(i * step + j * fine, fine)
            dots = lax.dot_general(key_ref[rows, :], q4, (((1,), (1,)), ((), ())), preferred_element_type=F32)
            sq = jnp.zeros((fine, LANES), F32)
            for t in range(dim // LANES):
                k = key_ref[rows, t * LANES : (t + 1) * LANES].astype(F32)
                sq = sq + k * k
            s = (2.0 * dots - jnp.sum(sq, axis=1, keepdims=True)) * inv_tau
            top = jnp.max(s, axis=0, keepdims=True)
            e = jnp.exp(s - top)
            s_ref[rows, :] = e
            tops.append(top)
            totals.append(jnp.sum(e, axis=0, keepdims=True))
    top = functools.reduce(jnp.maximum, tops)
    shrink = [jnp.exp(t - top) for t in tops]
    total = sum(a * b for a, b in zip(shrink, totals))
    scale = 1.0 / total
    knn_lse = top + jnp.log(total)
    for i in range(2 * n_chunk):
        rows = pl.ds(i * fine, fine)
        parts = _split3(s_ref[rows, :] * (shrink[i] * scale))
        for k in range(3):
            for b in range(2):
                at = k * WIDE + b * LANES
                rhs_ref[rows, at : at + LANES] = parts[k] * mask_ref[rows, b * LANES : (b + 1) * LANES]

    row_lane = _iota((1, LANES), 1)
    in_knn = (row_lane >= float(STAT)) & (row_lane < float(STAT + 32))
    stats = jnp.where(in_knn, knn_lse, lse_row)
    stats = jnp.where(row_lane == float(COUNT), demand, stats)
    places = jnp.dot(hot_ref[...], place_ref[...], preferred_element_type=F32)
    in_pool = (row_lane >= float(CAP)) & (row_lane < float(CAP + POOL))
    pool_place = jnp.where(in_pool, jnp.sum(places, axis=0, keepdims=True), 0.0)
    pool_bucket = jnp.sum(jnp.where(places > 0.0, sub + 1.0, 0.0), axis=0, keepdims=True)
    pool_bucket = jnp.where(in_pool, pool_bucket, 0.0)
    pool_bucket = pltpu.roll(jnp.broadcast_to(pool_bucket, (8, LANES)), POOL, 1)[:1]
    send[ROWS] = jnp.where(lane < float(CAP), places, 0.0) + (stats + pool_place + pool_bucket)
    for g in range(PARTS):
        base = g * (pool_at + 16)
        span = pool_at + (16 if g == 0 else 0)
        packed = jnp.dot(pack_ref[base : base + span, :], rhs_ref[...], preferred_element_type=F32)
        packed = packed[:, :WIDE] + packed[:, WIDE : 2 * WIDE] + packed[:, 2 * WIDE :]
        for r in range(DEPTH):
            for b in range(2):
                send[2 * r + b, g * group_len : (g + 1) * group_len] = packed[
                    r * group_len : (r + 1) * group_len, b * LANES : (b + 1) * LANES
                ]
        if g == 0:
            send[2 * DEPTH] = jnp.broadcast_to(packed[pool_at : pool_at + 1, :LANES], (n_dev, LANES))
            pl.semaphore_wait(barrier, n_dev - 1)
        for o in range(group_len):
            turn = (o * 29 + 29) % group_len
            if PARTS * turn + g == 0:
                continue
            pltpu.make_async_remote_copy(
                send.at[:, g * group_len + turn], recv.at[:, me], send_sem, recv_sem.at[me // half_len],
                device_id={"model": lax.rem(me + (PARTS * turn + g), n_dev)}, device_id_type=MESH,
            ).start()
    recv[:, pl.ds(me, 1), :] = send[:, 0:1, :]

    vocab = (_iota((WIDE, LANES), 0) + 1.0).astype(BF16)
    n_pair = (ROWS + 1) // 2
    peaks, sums, hists = [], [], []
    for h in range(HALF):
        inside = me // half_len == h

        @pl.when(inside)
        def _():
            landed = recv.at[:, pl.ds(0, half_len - 1)]
            pltpu.make_async_copy(landed, landed, recv_sem.at[h]).wait()

        @pl.when(jnp.logical_not(inside))
        def _():
            landed = recv.at[:, pl.ds(0, half_len)]
            pltpu.make_async_copy(landed, landed, recv_sem.at[h]).wait()

        span = slice(h * half_len, (h + 1) * half_len)
        meta = recv[ROWS, span]
        peak = jnp.max(meta, axis=0, keepdims=True)
        grown = jnp.exp(meta - peak)
        peaks.append(peak)
        sums.append(jnp.sum(grown, axis=0, keepdims=True))
        share = jnp.where(in_knn, grown, 0.0)
        share = share + pltpu.roll(share, 64, 1)
        share = share + pltpu.roll(share, 32, 1)
        by_lane = jnp.transpose(jnp.concatenate([meta, meta], axis=0))
        from_lane = lax.rem(lax.broadcasted_iota(jnp.int32, (1, LANES), 1), half_len) + h * half_len
        my_bucket = _bucket(me_f, from_lane.astype(F32), n_dev) + 1.0
        first_half = row_lane < float(half_len)
        for pair in range(n_pair):
            a, b = 2 * pair, 2 * pair + 1
            xa = recv[a, span] * share
            xb = recv[b, span] * share if b < ROWS else jnp.zeros_like(xa)
            parts = _split3(jnp.transpose(jnp.concatenate([xa, xb], axis=0)))
            for j in range(4):
                at = (j * n_pair + pair) * LANES
                for k in range(3):
                    x_ref[h, k * n_rows : (k + 1) * n_rows, at : at + LANES] = parts[k][j * n_rows : (j + 1) * n_rows]
                place_a = by_lane[4 * a + j : 4 * a + j + 1]
                if b < ROWS:
                    place_b = by_lane[4 * b + j : 4 * b + j + 1]
                else:
                    place_a = jnp.where(by_lane[CAP + POOL + j : CAP + POOL + j + 1] == my_bucket, place_a, 0.0)
                    place_b = jnp.zeros_like(place_a)
                wanted = jnp.broadcast_to(jnp.where(first_half, place_a, place_b), (WIDE, LANES)).astype(BF16)
                found_ref[h, :, at : at + LANES] = jnp.where(vocab == wanted, jnp.ones((), BF16), jnp.zeros((), BF16))
        hist = jnp.zeros((n_rows, WIDE), F32)
        cut = 2 * n_pair * LANES
        for j in range(2):
            got = lax.dot_general(
                x_ref[h, :, j * cut : (j + 1) * cut], found_ref[h, :, j * cut : (j + 1) * cut],
                (((1,), (1,)), ((), ())), preferred_element_type=F32,
            )
            hist = hist + (got[:n_rows] + got[n_rows : 2 * n_rows] + got[2 * n_rows :])
        hists.append(hist)
    peak = functools.reduce(jnp.maximum, peaks)
    shrink = [jnp.exp(p - peak) for p in peaks]
    total = sum(a * b for a, b in zip(shrink, sums))
    lse = peak + jnp.log(total)
    lse_col = jnp.sum(jnp.where(lm_diag, lse, 0.0), axis=1, keepdims=True)
    p_lm = (1.0 - mix_ref[0]) * jnp.exp(logits - lse_col)
    share = mix_ref[0] / total
    p_knn = sum(
        a * jnp.sum(jnp.where(knn_diag, s * share, 0.0), axis=1, keepdims=True) for a, s in zip(hists, shrink)
    )[:, :v_loc]
    if whole:
        outs[0][...] = jnp.log(p_knn + p_lm)
    else:
        outs[0][...] = p_knn
        outs[1][...] = p_lm
    most = jnp.max(jnp.where(row_lane == float(COUNT), peak, 0.0), axis=1, keepdims=True)
    outs[-1][...] = jnp.broadcast_to(most, (1, LANES))

    mine = send.at[:, pl.ds(0, n_dev - 1)]
    pltpu.make_async_copy(mine, mine, send_sem).wait()


def solution(mesh):
    n_dev = mesh.shape["model"]

    def local_step(queries, w_shard, key_shard, tok_shard, temperature, mix_weight):
        n_rows, dim = queries.shape
        n_keys, v_loc = key_shard.shape[0], w_shard.shape[1]
        tok = tok_shard.reshape(n_keys // LANES, LANES)
        any_space = pl.BlockSpec(memory_space=pl.ANY)
        smem = pl.BlockSpec(memory_space=pltpu.SMEM)
        vmem = pl.BlockSpec(memory_space=pltpu.VMEM)
        n_chunk = 4
        n_pair = (ROWS + 1) // 2

        def exchange(whole, r):
            block = jax.ShapeDtypeStruct((n_rows, v_loc), F32)
            shapes = [block] if whole else [block, block]
            return pl.pallas_call(
                functools.partial(_kernel, n_dev, whole),
                out_shape=shapes + [jax.ShapeDtypeStruct((1, LANES), F32)],
                in_specs=[smem] + [any_space] * 6,
                out_specs=[vmem] * (len(shapes) + 1),
                scratch_shapes=[
                    pltpu.SMEM((1,), F32),
                    pltpu.SMEM((1,), F32),
                    pltpu.VMEM((n_rows, dim), BF16),
                    pltpu.VMEM((dim, v_loc), BF16),
                    pltpu.VMEM((n_keys, dim), BF16),
                    pltpu.VMEM((n_keys // LANES, LANES), jnp.int32),
                    pltpu.VMEM((n_dev, n_keys), BF16),
                    pltpu.VMEM((DEPTH * n_dev + 16, n_keys), BF16),
                    pltpu.VMEM((n_keys, LANES), BF16),
                    pltpu.VMEM((n_keys, 3 * WIDE), BF16),
                    pltpu.VMEM((n_keys, LANES), F32),
                    pltpu.VMEM((n_keys, WIDE), BF16),
                    pltpu.VMEM((ROWS + 1, n_dev, LANES), F32),
                    pltpu.VMEM((ROWS + 1, n_dev, LANES), F32),
                    pltpu.VMEM((HALF, 3 * n_rows, 4 * n_pair * LANES), BF16),
                    pltpu.VMEM((HALF, WIDE, 4 * n_pair * LANES), BF16),
                    pltpu.SemaphoreType.DMA((5,)),
                    pltpu.SemaphoreType.DMA((n_chunk,)),
                    pltpu.SemaphoreType.DMA,
                    pltpu.SemaphoreType.DMA((HALF,)),
                ],
                compiler_params=pltpu.CompilerParams(
                    collective_id=0 if whole else 1, has_side_effects=True, vmem_limit_bytes=60 * 1024 * 1024
                ),
            )(r.reshape(1), temperature, mix_weight, queries, w_shard, key_shard, tok)

        out, demand = exchange(True, jnp.int32(0))

        def in_rounds(unused):
            zero = jnp.zeros((n_rows, v_loc), F32)

            def step(carry):
                r, unused, p_knn, unused_lm = carry
                more, p_lm, biggest = exchange(False, r)
                return r + 1, biggest[0, 0], p_knn + more, p_lm

            state = (jnp.int32(0), jnp.float32(1), zero, zero)
            state = lax.while_loop(lambda carry: (carry[0] * CAP).astype(F32) < carry[1], step, state)
            return jnp.log(state[2] + state[3])

        return lax.cond(demand[0, 0] > float(POOL), in_rounds, lambda done: done, out)

    return jax.shard_map(
        local_step,
        mesh=mesh,
        in_specs=(P("data", None), P(None, "model"), P("model", None), P("model"), P(), P()),
        out_specs=P("data", "model"),
        check_vma=False,
    )
```

```python
import functools

import jax
import jax.numpy as jnp
from jax import lax
from jax.experimental import pallas as pl
from jax.experimental.pallas import tpu as pltpu
from jax.sharding import PartitionSpec as P

MESH = pl.DeviceIdType.MESH
F32 = jnp.float32
BF16 = jnp.bfloat16
LANES = 128
WIDE = 2 * LANES
DEPTH = 4
CAP = 8 * DEPTH
POOL = 4
ROWS = 2 * DEPTH + 1
PARTS = 2
HALF = 2
COUNT = 48
STAT = 64
EMPTY = 255.0
CHUNKS = (512, 512, 512, 512)
SORTED = (8, 12, 16, 16)
FINE = 256


def _iota(shape, dim):
    return lax.broadcasted_iota(jnp.int32, shape, dim).astype(F32)


def _split3(x):
    hi = x.astype(BF16)
    rest = x - hi.astype(F32)
    mid = rest.astype(BF16)
    low = (rest - mid.astype(F32)).astype(BF16)
    return hi, mid, low


def _bucket(turn, n_dev):
    return lax.rem(turn, PARTS) * (n_dev // PARTS) + lax.div(turn, PARTS)


def _kernel(n_dev, whole, rnd_ref, tau_hbm, mix_hbm, q_hbm, w_hbm, key_hbm, tok_hbm, *refs):
    outs, refs = (refs[:2], refs[2:]) if whole else (refs[:3], refs[3:])
    (
        tau_ref, mix_ref, q_ref, w_ref, key_ref, tok_ref, hot_ref, pack_ref, place_ref, rhs_ref, s_ref, mask_ref,
        fac_ref, send, recv, x_ref, found_ref, in_sem, key_sem, send_sem, recv_sem,
    ) = refs
    me = lax.axis_index("model")
    n_rows, dim = q_ref.shape
    n_keys = key_ref.shape[1]
    v_loc = w_ref.shape[1]
    n_blk = n_keys // LANES
    n_tile = dim // LANES
    starts = [sum(CHUNKS[:i]) for i in range(len(CHUNKS))]
    group_len = n_dev // PARTS
    half_len = n_dev // HALF
    pool_at = DEPTH * group_len

    sources = [(tok_hbm, tok_ref), (q_hbm, q_ref), (w_hbm, w_ref), (tau_hbm, tau_ref), (mix_hbm, mix_ref)]
    loads = [pltpu.make_async_copy(src, dst, in_sem.at[i]) for i, (src, dst) in enumerate(sources)]
    for load in loads:
        load.start()
    for i, (at, size) in enumerate(zip(starts, CHUNKS)):
        for t in range(n_tile):
            pltpu.make_async_copy(
                key_hbm.at[pl.ds(at, size), pl.ds(t * LANES, LANES)], key_ref.at[t, pl.ds(at, size)], key_sem.at[i]
            ).start()

    barrier = pltpu.get_barrier_semaphore()
    for o in range(1, n_dev):
        pl.semaphore_signal(barrier, inc=1, device_id={"model": jnp.bitwise_xor(me, o)}, device_id_type=MESH)

    loads[0].wait()
    tok = tok_ref[...].astype(F32)
    owner = jnp.floor((tok + 0.5) * (1.0 / v_loc))
    place = tok - owner * v_loc + 1.0
    bucket = _bucket(jnp.bitwise_xor(owner.astype(jnp.int32), me), n_dev).astype(F32)
    sub = _iota((LANES, LANES), 0)
    lane = _iota((LANES, LANES), 1)
    ones = jnp.ones((LANES, LANES), BF16)
    upper = jnp.where(sub <= lane, 1.0, 0.0).astype(BF16)
    tri = jnp.concatenate([upper, ones], axis=1)
    for c in range(n_blk):
        hot_ref[c] = jnp.where(sub == bucket[c : c + 1, :], 1.0, 0.0).astype(BF16)
    ranks = []
    for c in range(0, n_blk, 4):
        hot_rows = jnp.concatenate([hot_ref[k] for k in range(c, c + 4)], axis=0)
        part = jnp.dot(hot_rows, tri, preferred_element_type=F32)
        ranks += [part[k * LANES : (k + 1) * LANES] for k in range(4)]
    before = jnp.zeros((LANES, LANES), F32)
    first = 1.0 if whole else rnd_ref[0].astype(F32) * float(CAP) + 1.0
    slots = []
    for c in range(n_blk):
        mine = sub == bucket[c : c + 1, :]
        slots.append(jnp.sum(jnp.where(mine, ranks[c][:, :LANES] + before, 0.0), axis=0, keepdims=True) - first)
        before = before + ranks[c][:, LANES:]
    slot = jnp.concatenate(slots, axis=0)
    if whole:
        over = jnp.where(slot >= float(CAP), 1.0, 0.0)
        inside = jnp.dot(over.astype(BF16), tri, preferred_element_type=F32)
        lower = jnp.where(_iota((n_blk, n_blk), 0) > _iota((n_blk, n_blk), 1), 1.0, 0.0).astype(BF16)
        ahead = jnp.dot(lower, inside[:, LANES:].astype(BF16), preferred_element_type=F32)
        rank = ahead + inside[:, :LANES] - 1.0
        code = jnp.where(rank < float(POOL), rank + float(CAP), EMPTY)
        code = jnp.where(slot < float(CAP), slot, code)
        demand = (ahead + inside[:, LANES:])[n_blk - 1 : n_blk]
    else:
        code = jnp.where((slot >= 0.0) & (slot < float(CAP)), slot, EMPTY)
        demand = jnp.max(before, axis=0, keepdims=True)
    depth = jnp.floor(code * 0.125)
    lane_group = jnp.floor(lane * (1.0 / 32.0))

    columns = jnp.transpose(jnp.concatenate([code, place] + [code] * (LANES // n_blk - 2), axis=0))

    def sort_block(c):
        rows = pl.ds(c * LANES, LANES)
        code_col = jnp.broadcast_to(columns[:, c : c + 1], (LANES, LANES))
        place_col = jnp.broadcast_to(columns[:, n_blk + c : n_blk + c + 1], (LANES, LANES))
        place_ref[rows, :] = jnp.where(code_col == lane, place_col, 0.0).astype(BF16)
        eighth = code_col - 8.0 * jnp.floor(code_col * 0.125)
        mask_ref[0, rows, :] = jnp.where(eighth == lane_group, 1.0, 0.0).astype(BF16)
        mask_ref[1, rows, :] = jnp.where(eighth == lane_group + 4.0, 1.0, 0.0).astype(BF16)
        hot = hot_ref[c]
        for r in range(DEPTH):
            keep = jnp.broadcast_to(jnp.where(depth[c : c + 1, :] == float(r), 1.0, 0.0), (LANES, LANES)).astype(BF16)
            kept = hot * keep
            for g in range(PARTS):
                at = g * (pool_at + 16) + r * group_len
                pack_ref[c, at : at + group_len] = kept[g * group_len : (g + 1) * group_len]
        spare = jnp.where((depth[c : c + 1, :] == float(DEPTH)) & (_iota((16, LANES), 0) == 0.0), 1.0, 0.0)
        pack_ref[c, pool_at : pool_at + 16] = spare.astype(BF16)

    for load in loads[1:]:
        load.wait()
    q = q_ref[...]
    logits = jnp.dot(q, w_ref[...], preferred_element_type=F32)
    lm_max = jnp.max(logits, axis=1, keepdims=True)
    lm_lse = lm_max + jnp.log(jnp.sum(jnp.exp(logits - lm_max), axis=1, keepdims=True))
    q_sub = _iota((n_rows, LANES), 0)
    q_lane = _iota((n_rows, LANES), 1)
    knn_diag = q_lane == q_sub + float(STAT)
    lm_diag = q_lane == q_sub + float(STAT + 32)
    lse_row = jnp.sum(jnp.where(lm_diag, lm_lse, 0.0), axis=0, keepdims=True)

    q4 = jnp.concatenate([q, q, q, q], axis=0)
    inv_tau = 1.0 / jnp.broadcast_to(tau_ref[...], (1, LANES))
    tops, totals = [], []

    def dots(i):
        for j in range(2):
            rows = pl.ds(starts[i] + j * CHUNKS[i] // 2, CHUNKS[i] // 2)
            keys = jnp.concatenate([key_ref[t, rows, :] for t in range(n_tile)], axis=1)
            s_ref[rows, :] = lax.dot_general(keys, q4, (((1,), (1,)), ((), ())), preferred_element_type=F32)

    def weigh(i):
        for j in range(CHUNKS[i] // FINE):
            rows = pl.ds(starts[i] + j * FINE, FINE)
            sq = jnp.zeros((FINE, LANES), F32)
            for t in range(n_tile):
                k = key_ref[t, rows, :].astype(F32)
                sq = sq + k * k
            s = (2.0 * s_ref[rows, :] - jnp.sum(sq, axis=1, keepdims=True)) * inv_tau
            top = jnp.max(s, axis=0, keepdims=True)
            e = jnp.exp(s - top)
            s_ref[rows, :] = e
            tops.append(top)
            totals.append(jnp.sum(e, axis=0, keepdims=True))

    sorted_up_to = 0
    for i in range(len(CHUNKS)):
        landed = key_ref.at[:, pl.ds(starts[i], CHUNKS[i])]
        pltpu.make_async_copy(landed, landed, key_sem.at[i]).wait()
        dots(i)
        for c in range(sorted_up_to, SORTED[i]):
            sort_block(c)
        sorted_up_to = SORTED[i]
        if i:
            weigh(i - 1)
    weigh(len(CHUNKS) - 1)
    top = functools.reduce(jnp.maximum, tops)
    shrink = [jnp.exp(t - top) for t in tops]
    total = sum(a * b for a, b in zip(shrink, totals))
    scale = 1.0 / total
    knn_lse = top + jnp.log(total)
    for i in range(n_keys // FINE):
        fac_ref[i] = jnp.broadcast_to(shrink[i] * scale, (8, LANES))

    def divide(i, carry):
        rows = pl.ds(pl.multiple_of(i * FINE, FINE), FINE)
        parts = _split3(s_ref[rows, :] * fac_ref[i][:1])
        for k in range(3):
            for m in range(2):
                rhs_ref[2 * k + m, rows, :] = parts[k] * mask_ref[m, rows, :]
        return carry

    lax.fori_loop(0, n_keys // FINE, divide, 0)

    row_lane = _iota((1, LANES), 1)
    in_knn = (row_lane >= float(STAT)) & (row_lane < float(STAT + 32))
    stats = jnp.where(in_knn, knn_lse, lse_row)
    stats = jnp.where(row_lane == float(COUNT), demand, stats)
    hot = jnp.concatenate([hot_ref[c] for c in range(n_blk)], axis=1)
    places = jnp.dot(hot, place_ref[...], preferred_element_type=F32)
    in_pool = (row_lane >= float(CAP)) & (row_lane < float(CAP + POOL))
    pool_place = jnp.where(in_pool, jnp.sum(places, axis=0, keepdims=True), 0.0)
    pool_bucket = jnp.sum(jnp.where(places > 0.0, sub + 1.0, 0.0), axis=0, keepdims=True)
    pool_bucket = jnp.where(in_pool, pool_bucket, 0.0)
    pool_bucket = pltpu.roll(jnp.broadcast_to(pool_bucket, (8, LANES)), POOL, 1)[:1]
    send[ROWS] = jnp.where(lane < float(CAP), places, 0.0) + (stats + pool_place + pool_bucket)
    for g in range(PARTS):
        base = g * (pool_at + 16)
        span = pool_at + (16 if g == 0 else 0)
        packed = []
        for lo, hi in ((0, pool_at // 2), (pool_at // 2, span)):
            lhs = jnp.concatenate([pack_ref[c, base + lo : base + hi, :] for c in range(n_blk)], axis=1)
            rhs = jnp.concatenate([rhs_ref[k] for k in range(6)], axis=1)
            got = jnp.dot(lhs, rhs, preferred_element_type=F32)
            packed.append(got[:, :WIDE] + got[:, WIDE : 2 * WIDE] + got[:, 2 * WIDE :])
        packed = jnp.concatenate(packed, axis=0)
        for r in range(DEPTH):
            for b in range(2):
                send[2 * r + b, g * group_len : (g + 1) * group_len] = packed[
                    r * group_len : (r + 1) * group_len, b * LANES : (b + 1) * LANES
                ]
        if g == 0:
            send[2 * DEPTH] = jnp.broadcast_to(packed[pool_at : pool_at + 1, :LANES], (n_dev, LANES))
            pl.semaphore_wait(barrier, n_dev - 1)
        for o in range(group_len):
            at = (o * 29 + 29) % group_len
            turn = PARTS * at + g
            if turn == 0:
                continue
            pltpu.make_async_remote_copy(
                send.at[:, g * group_len + at], recv.at[:, me], send_sem, recv_sem.at[me // half_len],
                device_id={"model": jnp.bitwise_xor(me, turn)}, device_id_type=MESH,
            ).start()
    recv[:, pl.ds(me, 1), :] = send[:, 0:1, :]

    vocab = (_iota((WIDE, LANES), 0) + 1.0).astype(BF16)
    n_pair = (ROWS + 1) // 2
    peaks, sums, hists = [], [], []
    for h in range(HALF):
        inside = me // half_len == h

        @pl.when(inside)
        def _():
            landed = recv.at[:, pl.ds(0, half_len - 1)]
            pltpu.make_async_copy(landed, landed, recv_sem.at[h]).wait()

        @pl.when(jnp.logical_not(inside))
        def _():
            landed = recv.at[:, pl.ds(0, half_len)]
            pltpu.make_async_copy(landed, landed, recv_sem.at[h]).wait()

        span = slice(h * half_len, (h + 1) * half_len)
        meta = recv[ROWS, span]
        peak = jnp.max(meta, axis=0, keepdims=True)
        grown = jnp.exp(meta - peak)
        peaks.append(peak)
        sums.append(jnp.sum(grown, axis=0, keepdims=True))
        share = jnp.where(in_knn, grown, 0.0)
        share = share + pltpu.roll(share, 64, 1)
        share = share + pltpu.roll(share, 32, 1)
        by_lane = jnp.transpose(jnp.concatenate([meta, meta], axis=0))
        from_lane = lax.rem(lax.broadcasted_iota(jnp.int32, (1, LANES), 1), half_len) + h * half_len
        my_bucket = _bucket(jnp.bitwise_xor(from_lane, me), n_dev).astype(F32) + 1.0
        first_half = row_lane < float(half_len)
        for pair in range(n_pair):
            a, b = 2 * pair, 2 * pair + 1
            xa = recv[a, span] * share
            xb = recv[b, span] * share if b < ROWS else jnp.zeros_like(xa)
            parts = _split3(jnp.transpose(jnp.concatenate([xa, xb], axis=0)))
            for j in range(4):
                at = j * n_pair + pair
                for k in range(3):
                    x_ref[h, at, k * n_rows : (k + 1) * n_rows] = parts[k][j * n_rows : (j + 1) * n_rows]
                place_a = by_lane[4 * a + j : 4 * a + j + 1]
                if b < ROWS:
                    place_b = by_lane[4 * b + j : 4 * b + j + 1]
                else:
                    place_a = jnp.where(by_lane[CAP + POOL + j : CAP + POOL + j + 1] == my_bucket, place_a, 0.0)
                    place_b = jnp.zeros_like(place_a)
                wanted = jnp.broadcast_to(jnp.where(first_half, place_a, place_b), (WIDE, LANES)).astype(BF16)
                found_ref[h, at] = jnp.where(vocab == wanted, jnp.ones((), BF16), jnp.zeros((), BF16))
        x = jnp.concatenate([x_ref[h, k] for k in range(4 * n_pair)], axis=1)
        hist = []
        for m in range(2):
            found = jnp.concatenate(
                [found_ref[h, k, m * LANES : (m + 1) * LANES] for k in range(4 * n_pair)], axis=1
            )
            got = lax.dot_general(x, found, (((1,), (1,)), ((), ())), preferred_element_type=F32)
            hist.append(got[:n_rows] + got[n_rows : 2 * n_rows] + got[2 * n_rows :])
        hist = jnp.concatenate(hist, axis=1)
        hists.append(hist)
    peak = functools.reduce(jnp.maximum, peaks)
    shrink = [jnp.exp(p - peak) for p in peaks]
    total = sum(a * b for a, b in zip(shrink, sums))
    lse = peak + jnp.log(total)
    lse_col = jnp.sum(jnp.where(lm_diag, lse, 0.0), axis=1, keepdims=True)
    p_lm = (1.0 - mix_ref[...]) * jnp.exp(logits - lse_col)
    share = mix_ref[...] / total
    p_knn = sum(
        a * jnp.sum(jnp.where(knn_diag, s * share, 0.0), axis=1, keepdims=True) for a, s in zip(hists, shrink)
    )[:, :v_loc]
    if whole:
        outs[0][...] = jnp.log(p_knn + p_lm)
    else:
        outs[0][...] = p_knn
        outs[1][...] = p_lm
    most = jnp.max(jnp.where(row_lane == float(COUNT), peak, 0.0), axis=1, keepdims=True)
    outs[-1][...] = jnp.broadcast_to(most, (1, LANES))

    mine = send.at[:, pl.ds(0, n_dev - 1)]
    pltpu.make_async_copy(mine, mine, send_sem).wait()


def solution(mesh):
    n_dev = mesh.shape["model"]

    def local_step(queries, w_shard, key_shard, tok_shard, temperature, mix_weight):
        n_rows, dim = queries.shape
        n_keys, v_loc = key_shard.shape[0], w_shard.shape[1]
        tok = tok_shard.reshape(n_keys // LANES, LANES)
        any_space = pl.BlockSpec(memory_space=pl.ANY)
        smem = pl.BlockSpec(memory_space=pltpu.SMEM)
        vmem = pl.BlockSpec(memory_space=pltpu.VMEM)
        n_pair = (ROWS + 1) // 2

        def exchange(whole, r):
            block = jax.ShapeDtypeStruct((n_rows, v_loc), F32)
            shapes = [block] if whole else [block, block]
            return pl.pallas_call(
                functools.partial(_kernel, n_dev, whole),
                out_shape=shapes + [jax.ShapeDtypeStruct((1, LANES), F32)],
                in_specs=[smem] + [any_space] * 6,
                out_specs=[vmem] * (len(shapes) + 1),
                scratch_shapes=[
                    pltpu.VMEM((1, 1), F32),
                    pltpu.VMEM((1, 1), F32),
                    pltpu.VMEM((n_rows, dim), BF16),
                    pltpu.VMEM((dim, v_loc), BF16),
                    pltpu.VMEM((dim // LANES, n_keys, LANES), BF16),
                    pltpu.VMEM((n_keys // LANES, LANES), jnp.int32),
                    pltpu.VMEM((n_keys // LANES, n_dev, LANES), BF16),
                    pltpu.VMEM((n_keys // LANES, DEPTH * n_dev + 16, LANES), BF16),
                    pltpu.VMEM((n_keys, LANES), BF16),
                    pltpu.VMEM((6, n_keys, LANES), BF16),
                    pltpu.VMEM((n_keys, LANES), F32),
                    pltpu.VMEM((2, n_keys, LANES), BF16),
                    pltpu.VMEM((n_keys // FINE, 8, LANES), F32),
                    pltpu.VMEM((ROWS + 1, n_dev, LANES), F32),
                    pltpu.VMEM((ROWS + 1, n_dev, LANES), F32),
                    pltpu.VMEM((HALF, 4 * n_pair, 3 * n_rows, LANES), BF16),
                    pltpu.VMEM((HALF, 4 * n_pair, WIDE, LANES), BF16),
                    pltpu.SemaphoreType.DMA((5,)),
                    pltpu.SemaphoreType.DMA((len(CHUNKS),)),
                    pltpu.SemaphoreType.DMA,
                    pltpu.SemaphoreType.DMA((HALF,)),
                ],
                compiler_params=pltpu.CompilerParams(
                    collective_id=0 if whole else 1, has_side_effects=True, vmem_limit_bytes=60 * 1024 * 1024
                ),
            )(r.reshape(1), temperature.reshape(1, 1), mix_weight.reshape(1, 1), queries, w_shard, key_shard, tok)

        out, demand = exchange(True, jnp.int32(0))

        def in_rounds(unused):
            zero = jnp.zeros((n_rows, v_loc), F32)

            def step(carry):
                r, unused, p_knn, unused_lm = carry
                more, p_lm, biggest = exchange(False, r)
                return r + 1, biggest[0, 0], p_knn + more, p_lm

            state = (jnp.int32(0), jnp.float32(1), zero, zero)
            state = lax.while_loop(lambda carry: (carry[0] * CAP).astype(F32) < carry[1], step, state)
            return jnp.log(state[2] + state[3])

        return lax.cond(demand[0, 0] > float(POOL), in_rounds, lambda done: done, out)

    return jax.shard_map(
        local_step,
        mesh=mesh,
        in_specs=(P("data", None), P(None, "model"), P("model", None), P("model"), P(), P()),
        out_specs=P("data", "model"),
        check_vma=False,
    )
```

```python
import functools

import jax
import jax.numpy as jnp
from jax import lax
from jax.experimental import pallas as pl
from jax.experimental.pallas import tpu as pltpu
from jax.sharding import PartitionSpec as P

MESH = pl.DeviceIdType.MESH
F32 = jnp.float32
BF16 = jnp.bfloat16
LANES = 128
WIDE = 2 * LANES
DEPTH = 4
CAP = 8 * DEPTH
POOL = 8
ROWS = 2 * DEPTH + 2
PARTS = 2
HALF = 2
COUNT = 48
STAT = 64
EMPTY = 255.0
CHUNKS = (512, 512, 512, 512)
SORTED = (8, 12, 16, 16)
FINE = 256


def _iota(shape, dim):
    return lax.broadcasted_iota(jnp.int32, shape, dim).astype(F32)


def _split3(x):
    hi = x.astype(BF16)
    rest = x - hi.astype(F32)
    mid = rest.astype(BF16)
    low = (rest - mid.astype(F32)).astype(BF16)
    return hi, mid, low


def _bucket(turn, n_dev):
    return lax.rem(turn, PARTS) * (n_dev // PARTS) + lax.div(turn, PARTS)


def _kernel(n_dev, whole, rnd_ref, tau_hbm, mix_hbm, q_hbm, w_hbm, key_hbm, tok_hbm, *refs):
    outs, refs = (refs[:2], refs[2:]) if whole else (refs[:3], refs[3:])
    (
        tau_ref, mix_ref, q_ref, w_ref, key_ref, tok_ref, hot_ref, pack_ref, place_ref, rhs_ref, s_ref, mask_ref,
        fac_ref, send, recv, x_ref, found_ref, in_sem, key_sem, send_sem, recv_sem,
    ) = refs
    me = lax.axis_index("model")
    n_rows, dim = q_ref.shape
    n_keys = key_ref.shape[1]
    v_loc = w_ref.shape[1]
    n_blk = n_keys // LANES
    n_tile = dim // LANES
    starts = [sum(CHUNKS[:i]) for i in range(len(CHUNKS))]
    group_len = n_dev // PARTS
    half_len = n_dev // HALF
    pool_at = DEPTH * group_len

    sources = [(tok_hbm, tok_ref), (q_hbm, q_ref), (w_hbm, w_ref), (tau_hbm, tau_ref), (mix_hbm, mix_ref)]
    loads = [pltpu.make_async_copy(src, dst, in_sem.at[i]) for i, (src, dst) in enumerate(sources)]
    for load in loads:
        load.start()
    for i, (at, size) in enumerate(zip(starts, CHUNKS)):
        for t in range(n_tile):
            pltpu.make_async_copy(
                key_hbm.at[pl.ds(at, size), pl.ds(t * LANES, LANES)], key_ref.at[t, pl.ds(at, size)], key_sem.at[i]
            ).start()

    barrier = pltpu.get_barrier_semaphore()
    for o in range(1, n_dev):
        pl.semaphore_signal(barrier, inc=1, device_id={"model": jnp.bitwise_xor(me, o)}, device_id_type=MESH)

    loads[0].wait()
    tok = tok_ref[...].astype(F32)
    owner = jnp.floor((tok + 0.5) * (1.0 / v_loc))
    place = tok - owner * v_loc + 1.0
    bucket = _bucket(jnp.bitwise_xor(owner.astype(jnp.int32), me), n_dev).astype(F32)
    sub = _iota((LANES, LANES), 0)
    lane = _iota((LANES, LANES), 1)
    ones = jnp.ones((LANES, LANES), BF16)
    upper = jnp.where(sub <= lane, 1.0, 0.0).astype(BF16)
    tri = jnp.concatenate([upper, ones], axis=1)
    for c in range(n_blk):
        hot_ref[c] = jnp.where(sub == bucket[c : c + 1, :], 1.0, 0.0).astype(BF16)
    ranks = []
    for c in range(0, n_blk, 4):
        hot_rows = jnp.concatenate([hot_ref[k] for k in range(c, c + 4)], axis=0)
        part = jnp.dot(hot_rows, tri, preferred_element_type=F32)
        ranks += [part[k * LANES : (k + 1) * LANES] for k in range(4)]
    before = jnp.zeros((LANES, LANES), F32)
    first = 1.0 if whole else rnd_ref[0].astype(F32) * float(CAP) + 1.0
    slots = []
    for c in range(n_blk):
        mine = sub == bucket[c : c + 1, :]
        slots.append(jnp.sum(jnp.where(mine, ranks[c][:, :LANES] + before, 0.0), axis=0, keepdims=True) - first)
        before = before + ranks[c][:, LANES:]
    slot = jnp.concatenate(slots, axis=0)
    if whole:
        over = jnp.where(slot >= float(CAP), 1.0, 0.0)
        inside = jnp.dot(over.astype(BF16), tri, preferred_element_type=F32)
        lower = jnp.where(_iota((n_blk, n_blk), 0) > _iota((n_blk, n_blk), 1), 1.0, 0.0).astype(BF16)
        ahead = jnp.dot(lower, inside[:, LANES:].astype(BF16), preferred_element_type=F32)
        rank = ahead + inside[:, :LANES] - 1.0
        code = jnp.where(rank < float(POOL), rank + float(CAP), EMPTY)
        code = jnp.where(slot < float(CAP), slot, code)
        demand = (ahead + inside[:, LANES:])[n_blk - 1 : n_blk]
    else:
        code = jnp.where((slot >= 0.0) & (slot < float(CAP)), slot, EMPTY)
        demand = jnp.max(before, axis=0, keepdims=True)
    depth = jnp.floor(code * 0.125)
    lane_group = jnp.floor(lane * (1.0 / 32.0))

    columns = jnp.transpose(jnp.concatenate([code, place] + [code] * (LANES // n_blk - 2), axis=0))

    def sort_block(c):
        rows = pl.ds(c * LANES, LANES)
        code_col = jnp.broadcast_to(columns[:, c : c + 1], (LANES, LANES))
        place_col = jnp.broadcast_to(columns[:, n_blk + c : n_blk + c + 1], (LANES, LANES))
        place_ref[rows, :] = jnp.where(code_col == lane, place_col, 0.0).astype(BF16)
        eighth = code_col - 8.0 * jnp.floor(code_col * 0.125)
        mask_ref[0, rows, :] = jnp.where(eighth == lane_group, 1.0, 0.0).astype(BF16)
        mask_ref[1, rows, :] = jnp.where(eighth == lane_group + 4.0, 1.0, 0.0).astype(BF16)
        hot = hot_ref[c]
        for r in range(DEPTH):
            keep = jnp.broadcast_to(jnp.where(depth[c : c + 1, :] == float(r), 1.0, 0.0), (LANES, LANES)).astype(BF16)
            kept = hot * keep
            for g in range(PARTS):
                at = g * (pool_at + 16) + r * group_len
                pack_ref[c, at : at + group_len] = kept[g * group_len : (g + 1) * group_len]
        spare = jnp.where((depth[c : c + 1, :] == float(DEPTH)) & (_iota((16, LANES), 0) == 0.0), 1.0, 0.0)
        pack_ref[c, pool_at : pool_at + 16] = spare.astype(BF16)

    for load in loads[1:]:
        load.wait()
    q = q_ref[...]
    logits = jnp.dot(q, w_ref[...], preferred_element_type=F32)
    lm_max = jnp.max(logits, axis=1, keepdims=True)
    lm_lse = lm_max + jnp.log(jnp.sum(jnp.exp(logits - lm_max), axis=1, keepdims=True))
    q_sub = _iota((n_rows, LANES), 0)
    q_lane = _iota((n_rows, LANES), 1)
    knn_diag = q_lane == q_sub + float(STAT)
    lm_diag = q_lane == q_sub + float(STAT + 32)
    lse_row = jnp.sum(jnp.where(lm_diag, lm_lse, 0.0), axis=0, keepdims=True)

    q4 = jnp.concatenate([q, q, q, q], axis=0)
    inv_tau = 1.0 / jnp.broadcast_to(tau_ref[...], (1, LANES))
    tops, totals = [], []

    def dots(i):
        for j in range(2):
            rows = pl.ds(starts[i] + j * CHUNKS[i] // 2, CHUNKS[i] // 2)
            keys = jnp.concatenate([key_ref[t, rows, :] for t in range(n_tile)], axis=1)
            s_ref[rows, :] = lax.dot_general(keys, q4, (((1,), (1,)), ((), ())), preferred_element_type=F32)

    def weigh(i):
        for j in range(CHUNKS[i] // FINE):
            rows = pl.ds(starts[i] + j * FINE, FINE)
            sq = jnp.zeros((FINE, LANES), F32)
            for t in range(n_tile):
                k = key_ref[t, rows, :].astype(F32)
                sq = sq + k * k
            s = (2.0 * s_ref[rows, :] - jnp.sum(sq, axis=1, keepdims=True)) * inv_tau
            top = jnp.max(s, axis=0, keepdims=True)
            e = jnp.exp(s - top)
            s_ref[rows, :] = e
            tops.append(top)
            totals.append(jnp.sum(e, axis=0, keepdims=True))

    sorted_up_to = 0
    for i in range(len(CHUNKS)):
        landed = key_ref.at[:, pl.ds(starts[i], CHUNKS[i])]
        pltpu.make_async_copy(landed, landed, key_sem.at[i]).wait()
        dots(i)
        for c in range(sorted_up_to, SORTED[i]):
            sort_block(c)
        sorted_up_to = SORTED[i]
        if i:
            weigh(i - 1)
    weigh(len(CHUNKS) - 1)
    top = functools.reduce(jnp.maximum, tops)
    shrink = [jnp.exp(t - top) for t in tops]
    total = sum(a * b for a, b in zip(shrink, totals))
    scale = 1.0 / total
    knn_lse = top + jnp.log(total)
    for i in range(n_keys // FINE):
        fac_ref[i] = jnp.broadcast_to(shrink[i] * scale, (8, LANES))

    def divide(i, carry):
        rows = pl.ds(pl.multiple_of(i * FINE, FINE), FINE)
        parts = _split3(s_ref[rows, :] * fac_ref[i][:1])
        for k in range(3):
            for m in range(2):
                rhs_ref[2 * k + m, rows, :] = parts[k] * mask_ref[m, rows, :]
        return carry

    lax.fori_loop(0, n_keys // FINE, divide, 0)

    row_lane = _iota((1, LANES), 1)
    in_knn = (row_lane >= float(STAT)) & (row_lane < float(STAT + 32))
    stats = jnp.where(in_knn, knn_lse, lse_row)
    stats = jnp.where(row_lane == float(COUNT), demand, stats)
    hot = jnp.concatenate([hot_ref[c] for c in range(n_blk)], axis=1)
    places = jnp.dot(hot, place_ref[...], preferred_element_type=F32)
    in_pool = (row_lane >= float(CAP)) & (row_lane < float(CAP + POOL))
    pool_place = jnp.where(in_pool, jnp.sum(places, axis=0, keepdims=True), 0.0)
    pool_bucket = jnp.sum(jnp.where(places > 0.0, sub + 1.0, 0.0), axis=0, keepdims=True)
    pool_bucket = jnp.where(in_pool, pool_bucket, 0.0)
    pool_bucket = pltpu.roll(jnp.broadcast_to(pool_bucket, (8, LANES)), POOL, 1)[:1]
    send[ROWS] = jnp.where(lane < float(CAP), places, 0.0) + (stats + pool_place + pool_bucket)
    for g in range(PARTS):
        base = g * (pool_at + 16)
        span = pool_at + (16 if g == 0 else 0)
        packed = []
        for lo, hi in ((0, pool_at // 2), (pool_at // 2, span)):
            lhs = jnp.concatenate([pack_ref[c, base + lo : base + hi, :] for c in range(n_blk)], axis=1)
            rhs = jnp.concatenate([rhs_ref[k] for k in range(6)], axis=1)
            got = jnp.dot(lhs, rhs, preferred_element_type=F32)
            packed.append(got[:, :WIDE] + got[:, WIDE : 2 * WIDE] + got[:, 2 * WIDE :])
        packed = jnp.concatenate(packed, axis=0)
        for r in range(DEPTH):
            for b in range(2):
                send[2 * r + b, g * group_len : (g + 1) * group_len] = packed[
                    r * group_len : (r + 1) * group_len, b * LANES : (b + 1) * LANES
                ]
        if g == 0:
            for m in range(2):
                spare = packed[pool_at : pool_at + 1, m * LANES : (m + 1) * LANES]
                send[2 * DEPTH + m] = jnp.broadcast_to(spare, (n_dev, LANES))
            pl.semaphore_wait(barrier, n_dev - 1)
        for o in range(group_len):
            at = (o * 29 + 29) % group_len
            turn = PARTS * at + g
            if turn == 0:
                continue
            pltpu.make_async_remote_copy(
                send.at[:, g * group_len + at], recv.at[:, me], send_sem, recv_sem.at[me // half_len],
                device_id={"model": jnp.bitwise_xor(me, turn)}, device_id_type=MESH,
            ).start()
    recv[:, pl.ds(me, 1), :] = send[:, 0:1, :]

    vocab = (_iota((WIDE, LANES), 0) + 1.0).astype(BF16)
    n_pair = ROWS // 2
    peaks, sums, hists = [], [], []
    for h in range(HALF):
        inside = me // half_len == h

        @pl.when(inside)
        def _():
            landed = recv.at[:, pl.ds(0, half_len - 1)]
            pltpu.make_async_copy(landed, landed, recv_sem.at[h]).wait()

        @pl.when(jnp.logical_not(inside))
        def _():
            landed = recv.at[:, pl.ds(0, half_len)]
            pltpu.make_async_copy(landed, landed, recv_sem.at[h]).wait()

        span = slice(h * half_len, (h + 1) * half_len)
        meta = recv[ROWS, span]
        peak = jnp.max(meta, axis=0, keepdims=True)
        grown = jnp.exp(meta - peak)
        peaks.append(peak)
        sums.append(jnp.sum(grown, axis=0, keepdims=True))
        share = jnp.where(in_knn, grown, 0.0)
        share = share + pltpu.roll(share, 64, 1)
        share = share + pltpu.roll(share, 32, 1)
        by_lane = jnp.transpose(jnp.concatenate([meta, meta], axis=0))
        from_lane = lax.rem(lax.broadcasted_iota(jnp.int32, (1, LANES), 1), half_len) + h * half_len
        my_bucket = _bucket(jnp.bitwise_xor(from_lane, me), n_dev).astype(F32) + 1.0
        first_half = row_lane < float(half_len)
        for pair in range(n_pair):
            a, b = 2 * pair, 2 * pair + 1
            xa = recv[a, span] * share
            xb = recv[b, span] * share
            parts = _split3(jnp.transpose(jnp.concatenate([xa, xb], axis=0)))
            for j in range(4):
                at = j * n_pair + pair
                for k in range(3):
                    x_ref[h, at, k * n_rows : (k + 1) * n_rows] = parts[k][j * n_rows : (j + 1) * n_rows]
                place_a = by_lane[4 * a + j : 4 * a + j + 1]
                place_b = by_lane[4 * b + j : 4 * b + j + 1]
                if a == 2 * DEPTH:
                    place_a = jnp.where(by_lane[CAP + POOL + j : CAP + POOL + j + 1] == my_bucket, place_a, 0.0)
                    place_b = jnp.where(by_lane[CAP + POOL + 4 + j : CAP + POOL + 5 + j] == my_bucket, place_b, 0.0)
                wanted = jnp.broadcast_to(jnp.where(first_half, place_a, place_b), (WIDE, LANES)).astype(BF16)
                found_ref[h, at] = jnp.where(vocab == wanted, jnp.ones((), BF16), jnp.zeros((), BF16))
        x = jnp.concatenate([x_ref[h, k] for k in range(4 * n_pair)], axis=1)
        hist = []
        for m in range(2):
            found = jnp.concatenate(
                [found_ref[h, k, m * LANES : (m + 1) * LANES] for k in range(4 * n_pair)], axis=1
            )
            got = lax.dot_general(x, found, (((1,), (1,)), ((), ())), preferred_element_type=F32)
            hist.append(got[:n_rows] + got[n_rows : 2 * n_rows] + got[2 * n_rows :])
        hist = jnp.concatenate(hist, axis=1)
        hists.append(hist)
    peak = functools.reduce(jnp.maximum, peaks)
    shrink = [jnp.exp(p - peak) for p in peaks]
    total = sum(a * b for a, b in zip(shrink, sums))
    lse = peak + jnp.log(total)
    lse_col = jnp.sum(jnp.where(lm_diag, lse, 0.0), axis=1, keepdims=True)
    p_lm = (1.0 - mix_ref[...]) * jnp.exp(logits - lse_col)
    share = mix_ref[...] / total
    p_knn = sum(
        a * jnp.sum(jnp.where(knn_diag, s * share, 0.0), axis=1, keepdims=True) for a, s in zip(hists, shrink)
    )[:, :v_loc]
    if whole:
        outs[0][...] = jnp.log(p_knn + p_lm)
    else:
        outs[0][...] = p_knn
        outs[1][...] = p_lm
    most = jnp.max(jnp.where(row_lane == float(COUNT), peak, 0.0), axis=1, keepdims=True)
    outs[-1][...] = jnp.broadcast_to(most, (1, LANES))

    mine = send.at[:, pl.ds(0, n_dev - 1)]
    pltpu.make_async_copy(mine, mine, send_sem).wait()


def solution(mesh):
    n_dev = mesh.shape["model"]

    def local_step(queries, w_shard, key_shard, tok_shard, temperature, mix_weight):
        n_rows, dim = queries.shape
        n_keys, v_loc = key_shard.shape[0], w_shard.shape[1]
        tok = tok_shard.reshape(n_keys // LANES, LANES)
        any_space = pl.BlockSpec(memory_space=pl.ANY)
        smem = pl.BlockSpec(memory_space=pltpu.SMEM)
        vmem = pl.BlockSpec(memory_space=pltpu.VMEM)
        n_pair = ROWS // 2

        def exchange(whole, r):
            block = jax.ShapeDtypeStruct((n_rows, v_loc), F32)
            shapes = [block] if whole else [block, block]
            return pl.pallas_call(
                functools.partial(_kernel, n_dev, whole),
                out_shape=shapes + [jax.ShapeDtypeStruct((1, LANES), F32)],
                in_specs=[smem] + [any_space] * 6,
                out_specs=[vmem] * (len(shapes) + 1),
                scratch_shapes=[
                    pltpu.VMEM((1, 1), F32),
                    pltpu.VMEM((1, 1), F32),
                    pltpu.VMEM((n_rows, dim), BF16),
                    pltpu.VMEM((dim, v_loc), BF16),
                    pltpu.VMEM((dim // LANES, n_keys, LANES), BF16),
                    pltpu.VMEM((n_keys // LANES, LANES), jnp.int32),
                    pltpu.VMEM((n_keys // LANES, n_dev, LANES), BF16),
                    pltpu.VMEM((n_keys // LANES, DEPTH * n_dev + 16, LANES), BF16),
                    pltpu.VMEM((n_keys, LANES), BF16),
                    pltpu.VMEM((6, n_keys, LANES), BF16),
                    pltpu.VMEM((n_keys, LANES), F32),
                    pltpu.VMEM((2, n_keys, LANES), BF16),
                    pltpu.VMEM((n_keys // FINE, 8, LANES), F32),
                    pltpu.VMEM((ROWS + 1, n_dev, LANES), F32),
                    pltpu.VMEM((ROWS + 1, n_dev, LANES), F32),
                    pltpu.VMEM((HALF, 4 * n_pair, 3 * n_rows, LANES), BF16),
                    pltpu.VMEM((HALF, 4 * n_pair, WIDE, LANES), BF16),
                    pltpu.SemaphoreType.DMA((5,)),
                    pltpu.SemaphoreType.DMA((len(CHUNKS),)),
                    pltpu.SemaphoreType.DMA,
                    pltpu.SemaphoreType.DMA((HALF,)),
                ],
                compiler_params=pltpu.CompilerParams(
                    collective_id=0 if whole else 1, has_side_effects=True, vmem_limit_bytes=60 * 1024 * 1024
                ),
            )(r.reshape(1), temperature.reshape(1, 1), mix_weight.reshape(1, 1), queries, w_shard, key_shard, tok)

        out, demand = exchange(True, jnp.int32(0))

        def in_rounds(unused):
            zero = jnp.zeros((n_rows, v_loc), F32)

            def step(carry):
                r, unused, p_knn, unused_lm = carry
                more, p_lm, biggest = exchange(False, r)
                return r + 1, biggest[0, 0], p_knn + more, p_lm

            state = (jnp.int32(0), jnp.float32(1), zero, zero)
            state = lax.while_loop(lambda carry: (carry[0] * CAP).astype(F32) < carry[1], step, state)
            return jnp.log(state[2] + state[3])

        return lax.cond(demand[0, 0] > float(POOL), in_rounds, lambda done: done, out)

    return jax.shard_map(
        local_step,
        mesh=mesh,
        in_specs=(P("data", None), P(None, "model"), P("model", None), P("model"), P(), P()),
        out_specs=P("data", "model"),
        check_vma=False,
    )
```

```python
import functools

import jax
import jax.numpy as jnp
from jax import lax
from jax.experimental import pallas as pl
from jax.experimental.pallas import tpu as pltpu
from jax.sharding import PartitionSpec as P

MESH = pl.DeviceIdType.MESH
F32 = jnp.float32
BF16 = jnp.bfloat16
LANES = 128
WIDE = 2 * LANES
DEPTH = 4
CAP = 8 * DEPTH
POOL = 8
ROWS = 2 * DEPTH + 2
PARTS = 4
HALF = 2
COUNT = 48
STAT = 64
EMPTY = 255.0
CHUNKS = (512, 512, 512, 512)
SORTED = (8, 12, 16, 16)
FINE = 64


def _iota(shape, dim):
    return lax.broadcasted_iota(jnp.int32, shape, dim).astype(F32)


def _split3(x):
    hi = x.astype(BF16)
    rest = x - hi.astype(F32)
    mid = rest.astype(BF16)
    low = (rest - mid.astype(F32)).astype(BF16)
    return hi, mid, low


def _bucket(turn, n_dev):
    return lax.rem(turn, PARTS) * (n_dev // PARTS) + lax.div(turn, PARTS)


def _kernel(n_dev, whole, rnd_ref, tau_hbm, mix_hbm, q_hbm, w_hbm, key_hbm, tok_hbm, *refs):
    outs, refs = (refs[:2], refs[2:]) if whole else (refs[:3], refs[3:])
    (
        tau_ref, mix_ref, q_ref, w_ref, key_ref, tok_ref, hot_ref, pack_ref, place_ref, rhs_ref, s_ref, mask_ref,
        fac_ref, send, recv, x_ref, found_ref, in_sem, key_sem, send_sem, recv_sem,
    ) = refs
    me = lax.axis_index("model")
    n_rows, dim = q_ref.shape
    n_keys = key_ref.shape[1]
    v_loc = w_ref.shape[1]
    n_blk = n_keys // LANES
    n_tile = dim // LANES
    starts = [sum(CHUNKS[:i]) for i in range(len(CHUNKS))]
    group_len = n_dev // PARTS
    half_len = n_dev // HALF
    pool_at = DEPTH * group_len

    sources = [(tok_hbm, tok_ref), (q_hbm, q_ref), (w_hbm, w_ref), (tau_hbm, tau_ref), (mix_hbm, mix_ref)]
    loads = [pltpu.make_async_copy(src, dst, in_sem.at[i]) for i, (src, dst) in enumerate(sources)]
    for load in loads:
        load.start()
    for i, (at, size) in enumerate(zip(starts, CHUNKS)):
        for t in range(n_tile):
            pltpu.make_async_copy(
                key_hbm.at[pl.ds(at, size), pl.ds(t * LANES, LANES)], key_ref.at[t, pl.ds(at, size)], key_sem.at[i]
            ).start()

    barrier = pltpu.get_barrier_semaphore()
    for o in range(1, n_dev):
        pl.semaphore_signal(barrier, inc=1, device_id={"model": jnp.bitwise_xor(me, o)}, device_id_type=MESH)

    loads[0].wait()
    tok = tok_ref[...].astype(F32)
    owner = jnp.floor((tok + 0.5) * (1.0 / v_loc))
    place = tok - owner * v_loc + 1.0
    bucket = _bucket(jnp.bitwise_xor(owner.astype(jnp.int32), me), n_dev).astype(F32)
    sub = _iota((LANES, LANES), 0)
    lane = _iota((LANES, LANES), 1)
    ones = jnp.ones((LANES, LANES), BF16)
    upper = jnp.where(sub <= lane, 1.0, 0.0).astype(BF16)
    tri = jnp.concatenate([upper, ones], axis=1)
    for c in range(n_blk):
        hot_ref[c] = jnp.where(sub == bucket[c : c + 1, :], 1.0, 0.0).astype(BF16)
    ranks = []
    for c in range(0, n_blk, 4):
        hot_rows = jnp.concatenate([hot_ref[k] for k in range(c, c + 4)], axis=0)
        part = jnp.dot(hot_rows, tri, preferred_element_type=F32)
        ranks += [part[k * LANES : (k + 1) * LANES] for k in range(4)]
    before = jnp.zeros((LANES, LANES), F32)
    first = 1.0 if whole else rnd_ref[0].astype(F32) * float(CAP) + 1.0
    slots = []
    for c in range(n_blk):
        mine = sub == bucket[c : c + 1, :]
        slots.append(jnp.sum(jnp.where(mine, ranks[c][:, :LANES] + before, 0.0), axis=0, keepdims=True) - first)
        before = before + ranks[c][:, LANES:]
    slot = jnp.concatenate(slots, axis=0)
    if whole:
        over = jnp.where(slot >= float(CAP), 1.0, 0.0)
        inside = jnp.dot(over.astype(BF16), tri, preferred_element_type=F32)
        lower = jnp.where(_iota((n_blk, n_blk), 0) > _iota((n_blk, n_blk), 1), 1.0, 0.0).astype(BF16)
        ahead = jnp.dot(lower, inside[:, LANES:].astype(BF16), preferred_element_type=F32)
        rank = ahead + inside[:, :LANES] - 1.0
        code = jnp.where(rank < float(POOL), rank + float(CAP), EMPTY)
        code = jnp.where(slot < float(CAP), slot, code)
        demand = (ahead + inside[:, LANES:])[n_blk - 1 : n_blk]
    else:
        code = jnp.where((slot >= 0.0) & (slot < float(CAP)), slot, EMPTY)
        demand = jnp.max(before, axis=0, keepdims=True)
    depth = jnp.floor(code * 0.125)
    lane_group = jnp.floor(lane * (1.0 / 32.0))

    columns = jnp.transpose(jnp.concatenate([code, place] + [code] * (LANES // n_blk - 2), axis=0))

    def sort_block(c):
        rows = pl.ds(c * LANES, LANES)
        code_col = jnp.broadcast_to(columns[:, c : c + 1], (LANES, LANES))
        place_col = jnp.broadcast_to(columns[:, n_blk + c : n_blk + c + 1], (LANES, LANES))
        place_ref[rows, :] = jnp.where(code_col == lane, place_col, 0.0).astype(BF16)
        eighth = code_col - 8.0 * jnp.floor(code_col * 0.125)
        mask_ref[0, rows, :] = jnp.where(eighth == lane_group, 1.0, 0.0).astype(BF16)
        mask_ref[1, rows, :] = jnp.where(eighth == lane_group + 4.0, 1.0, 0.0).astype(BF16)
        hot = hot_ref[c]
        for r in range(DEPTH):
            keep = jnp.broadcast_to(jnp.where(depth[c : c + 1, :] == float(r), 1.0, 0.0), (LANES, LANES)).astype(BF16)
            kept = hot * keep
            for g in range(PARTS):
                at = g * (pool_at + 16) + r * group_len
                pack_ref[c, at : at + group_len] = kept[g * group_len : (g + 1) * group_len]
        spare = jnp.where((depth[c : c + 1, :] == float(DEPTH)) & (_iota((16, LANES), 0) == 0.0), 1.0, 0.0)
        pack_ref[c, pool_at : pool_at + 16] = spare.astype(BF16)

    for load in loads[1:]:
        load.wait()
    q = q_ref[...]
    logits = jnp.dot(q, w_ref[...], preferred_element_type=F32)
    lm_max = jnp.max(logits, axis=1, keepdims=True)
    lm_lse = lm_max + jnp.log(jnp.sum(jnp.exp(logits - lm_max), axis=1, keepdims=True))
    q_sub = _iota((n_rows, LANES), 0)
    q_lane = _iota((n_rows, LANES), 1)
    knn_diag = q_lane == q_sub + float(STAT)
    lm_diag = q_lane == q_sub + float(STAT + 32)
    lse_row = jnp.sum(jnp.where(lm_diag, lm_lse, 0.0), axis=0, keepdims=True)

    q4 = jnp.concatenate([q, q, q, q], axis=0)
    inv_tau = 1.0 / jnp.broadcast_to(tau_ref[...], (1, LANES))
    tops, totals = [], []

    def dots(i):
        for j in range(2):
            rows = pl.ds(starts[i] + j * CHUNKS[i] // 2, CHUNKS[i] // 2)
            keys = jnp.concatenate([key_ref[t, rows, :] for t in range(n_tile)], axis=1)
            s_ref[rows, :] = lax.dot_general(keys, q4, (((1,), (1,)), ((), ())), preferred_element_type=F32)

    def weigh(i):
        for j in range(CHUNKS[i] // FINE):
            rows = pl.ds(starts[i] + j * FINE, FINE)
            sq = jnp.zeros((FINE, LANES), F32)
            for t in range(n_tile):
                k = key_ref[t, rows, :].astype(F32)
                sq = sq + k * k
            s = (2.0 * s_ref[rows, :] - jnp.sum(sq, axis=1, keepdims=True)) * inv_tau
            top = jnp.max(s, axis=0, keepdims=True)
            e = jnp.exp(s - top)
            s_ref[rows, :] = e
            tops.append(top)
            totals.append(jnp.sum(e, axis=0, keepdims=True))

    sorted_up_to = 0
    for i in range(len(CHUNKS)):
        landed = key_ref.at[:, pl.ds(starts[i], CHUNKS[i])]
        pltpu.make_async_copy(landed, landed, key_sem.at[i]).wait()
        dots(i)
        for c in range(sorted_up_to, SORTED[i]):
            sort_block(c)
        sorted_up_to = SORTED[i]
        if i:
            weigh(i - 1)
    weigh(len(CHUNKS) - 1)
    top = functools.reduce(jnp.maximum, tops)
    shrink = [jnp.exp(t - top) for t in tops]
    total = sum(a * b for a, b in zip(shrink, totals))
    scale = 1.0 / total
    knn_lse = top + jnp.log(total)
    for i in range(n_keys // FINE):
        fac_ref[i] = jnp.broadcast_to(shrink[i] * scale, (8, LANES))

    def divide(i, carry):
        rows = pl.ds(pl.multiple_of(i * FINE, FINE), FINE)
        parts = _split3(s_ref[rows, :] * fac_ref[i][:1])
        for k in range(3):
            for m in range(2):
                rhs_ref[2 * k + m, rows, :] = parts[k] * mask_ref[m, rows, :]
        return carry

    lax.fori_loop(0, n_keys // FINE, divide, 0)

    row_lane = _iota((1, LANES), 1)
    in_knn = (row_lane >= float(STAT)) & (row_lane < float(STAT + 32))
    stats = jnp.where(in_knn, knn_lse, lse_row)
    stats = jnp.where(row_lane == float(COUNT), demand, stats)
    hot = jnp.concatenate([hot_ref[c] for c in range(n_blk)], axis=1)
    places = jnp.dot(hot, place_ref[...], preferred_element_type=F32)
    in_pool = (row_lane >= float(CAP)) & (row_lane < float(CAP + POOL))
    pool_place = jnp.where(in_pool, jnp.sum(places, axis=0, keepdims=True), 0.0)
    pool_bucket = jnp.sum(jnp.where(places > 0.0, sub + 1.0, 0.0), axis=0, keepdims=True)
    pool_bucket = jnp.where(in_pool, pool_bucket, 0.0)
    pool_bucket = pltpu.roll(jnp.broadcast_to(pool_bucket, (8, LANES)), POOL, 1)[:1]
    send[ROWS] = jnp.where(lane < float(CAP), places, 0.0) + (stats + pool_place + pool_bucket)
    for g in range(PARTS):
        base = g * (pool_at + 16)
        span = pool_at + (16 if g == 0 else 0)
        packed = []
        for lo, hi in ((0, pool_at // 2), (pool_at // 2, span)):
            lhs = jnp.concatenate([pack_ref[c, base + lo : base + hi, :] for c in range(n_blk)], axis=1)
            rhs = jnp.concatenate([rhs_ref[k] for k in range(6)], axis=1)
            got = jnp.dot(lhs, rhs, preferred_element_type=F32)
            packed.append(got[:, :WIDE] + got[:, WIDE : 2 * WIDE] + got[:, 2 * WIDE :])
        packed = jnp.concatenate(packed, axis=0)
        for r in range(DEPTH):
            for b in range(2):
                send[2 * r + b, g * group_len : (g + 1) * group_len] = packed[
                    r * group_len : (r + 1) * group_len, b * LANES : (b + 1) * LANES
                ]
        if g == 0:
            for m in range(2):
                spare = packed[pool_at : pool_at + 1, m * LANES : (m + 1) * LANES]
                send[2 * DEPTH + m] = jnp.broadcast_to(spare, (n_dev, LANES))
            pl.semaphore_wait(barrier, n_dev - 1)
        for o in range(group_len):
            at = (o * 29 + 29) % group_len
            turn = PARTS * at + g
            if turn == 0:
                continue
            pltpu.make_async_remote_copy(
                send.at[:, g * group_len + at], recv.at[:, me], send_sem, recv_sem.at[me // half_len],
                device_id={"model": jnp.bitwise_xor(me, turn)}, device_id_type=MESH,
            ).start()
    recv[:, pl.ds(me, 1), :] = send[:, 0:1, :]

    vocab = (_iota((WIDE, LANES), 0) + 1.0).astype(BF16)
    n_pair = ROWS // 2
    peaks, sums, hists = [], [], []
    for h in range(HALF):
        inside = me // half_len == h

        @pl.when(inside)
        def _():
            landed = recv.at[:, pl.ds(0, half_len - 1)]
            pltpu.make_async_copy(landed, landed, recv_sem.at[h]).wait()

        @pl.when(jnp.logical_not(inside))
        def _():
            landed = recv.at[:, pl.ds(0, half_len)]
            pltpu.make_async_copy(landed, landed, recv_sem.at[h]).wait()

        span = slice(h * half_len, (h + 1) * half_len)
        meta = recv[ROWS, span]
        peak = jnp.max(meta, axis=0, keepdims=True)
        grown = jnp.exp(meta - peak)
        peaks.append(peak)
        sums.append(jnp.sum(grown, axis=0, keepdims=True))
        share = jnp.where(in_knn, grown, 0.0)
        share = share + pltpu.roll(share, 64, 1)
        share = share + pltpu.roll(share, 32, 1)
        by_lane = jnp.transpose(jnp.concatenate([meta, meta], axis=0))
        from_lane = lax.rem(lax.broadcasted_iota(jnp.int32, (1, LANES), 1), half_len) + h * half_len
        my_bucket = _bucket(jnp.bitwise_xor(from_lane, me), n_dev).astype(F32) + 1.0
        first_half = row_lane < float(half_len)
        for pair in range(n_pair):
            a, b = 2 * pair, 2 * pair + 1
            xa = recv[a, span] * share
            xb = recv[b, span] * share
            parts = _split3(jnp.transpose(jnp.concatenate([xa, xb], axis=0)))
            for j in range(4):
                at = j * n_pair + pair
                for k in range(3):
                    x_ref[h, at, k * n_rows : (k + 1) * n_rows] = parts[k][j * n_rows : (j + 1) * n_rows]
                place_a = by_lane[4 * a + j : 4 * a + j + 1]
                place_b = by_lane[4 * b + j : 4 * b + j + 1]
                if a == 2 * DEPTH:
                    place_a = jnp.where(by_lane[CAP + POOL + j : CAP + POOL + j + 1] == my_bucket, place_a, 0.0)
                    place_b = jnp.where(by_lane[CAP + POOL + 4 + j : CAP + POOL + 5 + j] == my_bucket, place_b, 0.0)
                wanted = jnp.broadcast_to(jnp.where(first_half, place_a, place_b), (WIDE, LANES)).astype(BF16)
                found_ref[h, at] = jnp.where(vocab == wanted, jnp.ones((), BF16), jnp.zeros((), BF16))
        x = jnp.concatenate([x_ref[h, k] for k in range(4 * n_pair)], axis=1)
        hist = []
        for m in range(2):
            found = jnp.concatenate(
                [found_ref[h, k, m * LANES : (m + 1) * LANES] for k in range(4 * n_pair)], axis=1
            )
            got = lax.dot_general(x, found, (((1,), (1,)), ((), ())), preferred_element_type=F32)
            hist.append(got[:n_rows] + got[n_rows : 2 * n_rows] + got[2 * n_rows :])
        hist = jnp.concatenate(hist, axis=1)
        hists.append(hist)
    peak = functools.reduce(jnp.maximum, peaks)
    shrink = [jnp.exp(p - peak) for p in peaks]
    total = sum(a * b for a, b in zip(shrink, sums))
    lse = peak + jnp.log(total)
    lse_col = jnp.sum(jnp.where(lm_diag, lse, 0.0), axis=1, keepdims=True)
    p_lm = (1.0 - mix_ref[...]) * jnp.exp(logits - lse_col)
    share = mix_ref[...] / total
    p_knn = sum(
        a * jnp.sum(jnp.where(knn_diag, s * share, 0.0), axis=1, keepdims=True) for a, s in zip(hists, shrink)
    )[:, :v_loc]
    if whole:
        outs[0][...] = jnp.log(p_knn + p_lm)
    else:
        outs[0][...] = p_knn
        outs[1][...] = p_lm
    most = jnp.max(jnp.where(row_lane == float(COUNT), peak, 0.0), axis=1, keepdims=True)
    outs[-1][...] = jnp.broadcast_to(most, (1, LANES))

    mine = send.at[:, pl.ds(0, n_dev - 1)]
    pltpu.make_async_copy(mine, mine, send_sem).wait()


def solution(mesh):
    n_dev = mesh.shape["model"]

    def local_step(queries, w_shard, key_shard, tok_shard, temperature, mix_weight):
        n_rows, dim = queries.shape
        n_keys, v_loc = key_shard.shape[0], w_shard.shape[1]
        tok = tok_shard.reshape(n_keys // LANES, LANES)
        any_space = pl.BlockSpec(memory_space=pl.ANY)
        smem = pl.BlockSpec(memory_space=pltpu.SMEM)
        vmem = pl.BlockSpec(memory_space=pltpu.VMEM)
        n_pair = ROWS // 2

        def exchange(whole, r):
            block = jax.ShapeDtypeStruct((n_rows, v_loc), F32)
            shapes = [block] if whole else [block, block]
            return pl.pallas_call(
                functools.partial(_kernel, n_dev, whole),
                out_shape=shapes + [jax.ShapeDtypeStruct((1, LANES), F32)],
                in_specs=[smem] + [any_space] * 6,
                out_specs=[vmem] * (len(shapes) + 1),
                scratch_shapes=[
                    pltpu.VMEM((1, 1), F32),
                    pltpu.VMEM((1, 1), F32),
                    pltpu.VMEM((n_rows, dim), BF16),
                    pltpu.VMEM((dim, v_loc), BF16),
                    pltpu.VMEM((dim // LANES, n_keys, LANES), BF16),
                    pltpu.VMEM((n_keys // LANES, LANES), jnp.int32),
                    pltpu.VMEM((n_keys // LANES, n_dev, LANES), BF16),
                    pltpu.VMEM((n_keys // LANES, DEPTH * n_dev + 16 * (PARTS - 1), LANES), BF16),
                    pltpu.VMEM((n_keys, LANES), BF16),
                    pltpu.VMEM((6, n_keys, LANES), BF16),
                    pltpu.VMEM((n_keys, LANES), F32),
                    pltpu.VMEM((2, n_keys, LANES), BF16),
                    pltpu.VMEM((n_keys // FINE, 8, LANES), F32),
                    pltpu.VMEM((ROWS + 1, n_dev, LANES), F32),
                    pltpu.VMEM((ROWS + 1, n_dev, LANES), F32),
                    pltpu.VMEM((HALF, 4 * n_pair, 3 * n_rows, LANES), BF16),
                    pltpu.VMEM((HALF, 4 * n_pair, WIDE, LANES), BF16),
                    pltpu.SemaphoreType.DMA((5,)),
                    pltpu.SemaphoreType.DMA((len(CHUNKS),)),
                    pltpu.SemaphoreType.DMA,
                    pltpu.SemaphoreType.DMA((HALF,)),
                ],
                compiler_params=pltpu.CompilerParams(
                    collective_id=0 if whole else 1, has_side_effects=True, vmem_limit_bytes=60 * 1024 * 1024
                ),
            )(r.reshape(1), temperature.reshape(1, 1), mix_weight.reshape(1, 1), queries, w_shard, key_shard, tok)

        out, demand = exchange(True, jnp.int32(0))

        def in_rounds(unused):
            zero = jnp.zeros((n_rows, v_loc), F32)

            def step(carry):
                r, unused, p_knn, unused_lm = carry
                more, p_lm, biggest = exchange(False, r)
                return r + 1, biggest[0, 0], p_knn + more, p_lm

            state = (jnp.int32(0), jnp.float32(1), zero, zero)
            state = lax.while_loop(lambda carry: (carry[0] * CAP).astype(F32) < carry[1], step, state)
            return jnp.log(state[2] + state[3])

        return lax.cond(demand[0, 0] > float(POOL), in_rounds, lambda done: done, out)

    return jax.shard_map(
        local_step,
        mesh=mesh,
        in_specs=(P("data", None), P(None, "model"), P("model", None), P("model"), P(), P()),
        out_specs=P("data", "model"),
        check_vma=False,
    )
```
